128 devices in a mesh: rows: 8 (over y_lo, x), cols: 16 (over z, y_hi, core).
Axes of the slice: x: 4, y: 4 (y_hi: 2, y_lo: 2; y = y_hi * 2 + y_lo), z: 4, core: 2. Of those that a mesh axis runs over, the one named last changes fastest.
Arguments:
- heat_excess: float32 [8, 2048, 8192], P(None, ('rows', 'cols')), may hold values from -6 to 6
- square_region_label: int32 [2048, 8192], P(('rows', 'cols')), may hold values from 0 to 63
- region_heating_flux: float32 [64], replicated, may hold values from 0.05 to 0.5
- layer_substance_label: int32 [8], replicated, may hold values from 0 to 3, as said below
- sideways_coupling_factor: float32 [4], replicated, may hold values from 0.08 to 0.2
- upward_coupling_factor: float32 [4], replicated, may hold values from 0.02 to 0.08
- layer_heating_fraction: float32 [4], replicated, may hold values from 0.1 to 0.6
Outputs:
- ending_heat_excess: float32 [8, 2048, 8192], P(None, 'rows', 'cols')
The draws below stay inside these ranges and needn't reach their ends.
Inputs may be any that keep to these rules, and one draw needn't show every extreme that they name: `layer_substance_label`: each material is named by exactly 2 tiers.
All inputs are finite; a program needn't handle non-finite values.
Results may differ from the reference program's by a relative error of at most 0.00002.
Values sent between devices are 32-bit elements; how exact they have to be, the bound alone decides.
No kernel may reach another device: no remote copies, remote signals or barrier semaphores. Data moves between devices by JAX's collectives and lax.ppermute only.
A program may use at most 192 MiB of HBM per device.

```python
import math
import jax
import jax.numpy as jnp
from jax import lax

LAYER_COUNT = 8
NMAT = 4
NBLOCKS = 64
EPOCH_TOTAL = 8
MESH_HEIGHTWISE = 2048
MESH_WIDTHWISE = 8192


def draw_layer_substance_label(key, part):
    pieces = [jax.random.permutation(jax.random.fold_in(key, 7 + index), NMAT) for index in range(LAYER_COUNT // NMAT)]
    return jnp.concatenate(pieces).astype(jnp.int32)


def set_ends(entries, stream_key, least, top_value):
    index_at = [jax.random.randint(jax.random.fold_in(stream_key, axis), (), 0, length) for axis, length in enumerate(entries.shape)]
    longest = entries.shape.index(max(entries.shape))
    beside = index_at[:longest] + [(index_at[longest] + 1) % entries.shape[longest]] + index_at[longest + 1:]
    return entries.at[tuple(index_at)].set(least).at[tuple(beside)].set(top_value)


def levels(key, shape, shards, least, high):
    loudness, own = 1.0, jax.random.fold_in(key, 6)
    for dim, shards_of in shards:
        steps = jnp.exp(jax.random.uniform(jax.random.fold_in(own, dim), (shards_of,), jnp.float32, least / len(shards), high / len(shards)))
        loudness = loudness * jnp.repeat(steps, shape[dim] // shards_of).reshape([-1 if axis == dim else 1 for axis in range(len(shape))])
    return loudness


def centred(stream_key, dims, scale, most, cuts=(), dtype=jnp.bfloat16):
    drawn = jax.random.normal(stream_key, dims, jnp.float32) * scale
    if len(cuts) > 0:
        drawn = levels(stream_key, dims, cuts, -0.22, 0.18) * drawn
    return jnp.clip(drawn, min=-most, max=most).astype(dtype)


def setup_inputs(seed: int = 0) -> dict:
    key_of = jax.random.split(jax.random.key(seed), 8)
    heat_excess = centred(key_of[0], (LAYER_COUNT, MESH_HEIGHTWISE, MESH_WIDTHWISE), 1.0, 6.0, ((1, 128),), jnp.float32)
    square_region_label = set_ends(jax.random.randint(key_of[1], (MESH_HEIGHTWISE, MESH_WIDTHWISE), 0, NBLOCKS), jax.random.fold_in(key_of[1], 1), 0, NBLOCKS - 1).astype(jnp.int32)
    region_heating_flux = jnp.clip(jnp.exp(jax.random.uniform(key_of[2], (NBLOCKS,), jnp.float32, math.log(0.05), math.log(0.5))), 0.05, 0.5)
    layer_substance_label = draw_layer_substance_label(jax.random.fold_in(key_of[7], 71), 0)
    sideways_coupling_factor = jnp.clip(jax.random.uniform(key_of[4], (NMAT,), jnp.float32, 0.08, 0.2), 0.08, 0.2)
    upward_coupling_factor = jnp.clip(jax.random.uniform(key_of[5], (NMAT,), jnp.float32, 0.02, 0.08), 0.02, 0.08)
    layer_heating_fraction = jnp.clip(jax.random.uniform(key_of[6], (NMAT,), jnp.float32, 0.1, 0.6), 0.1, 0.6)
    return {"heat_excess": heat_excess, "square_region_label": square_region_label, "region_heating_flux": region_heating_flux, "layer_substance_label": layer_substance_label, "sideways_coupling_factor": sideways_coupling_factor, "upward_coupling_factor": upward_coupling_factor, "layer_heating_fraction": layer_heating_fraction}


def reference(heat_excess, square_region_label, region_heating_flux, layer_substance_label, sideways_coupling_factor, upward_coupling_factor, layer_heating_fraction):
    density = jnp.take(region_heating_flux, square_region_label, axis=0)
    lateral = jnp.take(sideways_coupling_factor, layer_substance_label, axis=0)[:, None, None]
    vertical = jnp.take(upward_coupling_factor, layer_substance_label, axis=0)[:, None, None]
    share = jnp.take(layer_heating_fraction, layer_substance_label, axis=0)[:, None, None]
    source = share * density[None]

    def advance_integrator(field, discarded_output):
        padded = jnp.pad(field, ((0, 0), (1, 1), (1, 1)))
        beside = padded[:, 2:, 1:-1] + padded[:, :-2, 1:-1]
        beside = beside + padded[:, 1:-1, 2:] + padded[:, 1:-1, :-2]
        above = jnp.concatenate([field[1:], jnp.zeros_like(field[:1])], axis=0)
        flux = vertical * (above - field)
        below = jnp.concatenate([jnp.zeros_like(flux[:1]), flux[:-1]], axis=0)
        fresh = field + lateral * (beside - 4.0 * field) + flux - below + source
        return fresh, None

    ending_heat_excess, discarded_output = lax.scan(advance_integrator, heat_excess, None, length=EPOCH_TOTAL)
    return ending_heat_excess
```

```python
import functools

import jax
import jax.numpy as jnp
from jax import lax
from jax.experimental import pallas as pl
from jax.experimental.pallas import tpu as pltpu
from jax.sharding import PartitionSpec as P

STEPS = 8
TIERS = 8
LANES = 128
EDGE = 16
VMEM = pltpu.MemorySpace.VMEM
SMEM = pltpu.MemorySpace.SMEM


def lane_index():
    return lax.broadcasted_iota(jnp.int32, (8, LANES), 1)


def pack_kernel(x_ref, label_ref, flux_ref, out_ref, table, density):
    targets = out_ref.shape[0]
    blocks = (out_ref.shape[1] - 2) // (TIERS + 1)
    rows = x_ref.shape[1]
    count = flux_ref.shape[1]
    table[:, :count] = jnp.broadcast_to(flux_ref[...], (8, count))
    look = table[...]
    lane = lane_index()
    group = lane // 16

    def fill(i, carry):
        at = pl.multiple_of(i * LANES, LANES)
        for r in range(0, rows, 8):
            ids = label_ref[r : r + 8, pl.ds(at, LANES)]
            density[r : r + 8, pl.ds(at, LANES)] = jnp.take_along_axis(look, ids, axis=1)
        return carry

    lax.fori_loop(0, density.shape[1] // LANES, fill, 0, unroll=4)

    def one(d, carry):
        first = d * blocks * LANES
        for b in range(blocks):
            at = pl.multiple_of(first + b * LANES, LANES)
            for k in range(TIERS):
                out_ref[d, k * blocks + b] = x_ref[k, :, pl.ds(at, LANES)]
            out_ref[d, TIERS * blocks + b] = density[:, pl.ds(at, LANES)]
        before = pl.multiple_of(jnp.maximum(first - LANES, 0), LANES)
        after = pl.multiple_of(jnp.minimum(first + blocks * LANES, x_ref.shape[2] - LANES), LANES)
        low, high = jnp.where(d < targets - 1, 0, 8), jnp.where(d > 0, LANES, 8)
        keep = jnp.logical_and(lane >= low, lane < high)
        for r in range(0, rows, 8):
            warm = jnp.zeros((8, LANES), jnp.float32)
            power = jnp.zeros((8, LANES), jnp.float32)
            ends = jnp.where(
                lane < 8, density[r : r + 8, pl.ds(after, LANES)], density[r : r + 8, pl.ds(before, LANES)]
            )
            ends = jnp.where(keep, ends, 0.0)
            for k in range(TIERS):
                both = jnp.where(
                    lane < 8, x_ref[k, r : r + 8, pl.ds(after, LANES)], x_ref[k, r : r + 8, pl.ds(before, LANES)]
                )
                both = jnp.where(keep, both, 0.0)
                turn = (16 * k + 8) % LANES
                warm = jnp.where(group == k, pltpu.roll(both, turn, 1), warm)
                power = jnp.where(group == k, pltpu.roll(ends, turn, 1), power)
            out_ref[d, (TIERS + 1) * blocks, r : r + 8] = warm
            out_ref[d, (TIERS + 1) * blocks + 1, r : r + 8] = power
        return carry

    lax.fori_loop(0, targets, one, 0)


def pack(x, labels, flux, targets, blocks):
    parts = (TIERS + 1) * blocks + 2
    return pl.pallas_call(
        pack_kernel,
        out_shape=jax.ShapeDtypeStruct((targets, parts, x.shape[1], LANES), jnp.float32),
        in_specs=[pl.BlockSpec(memory_space=VMEM)] * 3,
        out_specs=pl.BlockSpec(memory_space=VMEM),
        scratch_shapes=[
            pltpu.VMEM((8, LANES), jnp.float32),
            pltpu.VMEM(labels.shape, jnp.float32),
        ],
        compiler_params=pltpu.CompilerParams(vmem_limit_bytes=40 << 20),
    )(x, labels, flux)


def step_kernel(
    edge_ref, mat_ref, lat_ref, up_ref, heat_ref, got_ref, top_ref, low_ref, out_ref, t, s, dens, side, sems
):
    blocks = t.shape[2]
    sources, _, strip, _ = got_ref.shape
    height = sources * strip
    lane = lane_index()
    group = lane // 16
    inner = lane % 16
    at_top = edge_ref[0] == 1
    at_low = edge_ref[1] == 1

    lat = [lat_ref[mat_ref[k]] for k in range(TIERS)]
    ver = [up_ref[mat_ref[k]] for k in range(TIERS)]
    share = [heat_ref[mat_ref[k]] for k in range(TIERS)]
    own = [1.0 - 4.0 * lat[k] - ver[k] - (ver[k - 1] if k else 0.0) for k in range(TIERS)]

    def by_lane(values):
        full = jnp.zeros((8, LANES), jnp.float32)
        for k, value in enumerate(values):
            full = jnp.where(group == k, value, full)
        return full

    def place(n, carry):
        at = pl.multiple_of(EDGE + n * strip, 8)
        for b in range(blocks):
            for k in range(TIERS):
                t[0, k, b, pl.ds(at, strip)] = got_ref[n, k * blocks + b]
            dens[b, pl.ds(at, strip)] = got_ref[n, TIERS * blocks + b]
        for i in range(2):
            s[0, i, pl.ds(at, strip)] = got_ref[n, (TIERS + 1) * blocks]
            side[i, pl.ds(at, strip)] = got_ref[n, (TIERS + 1) * blocks + 1]
        return carry

    lax.fori_loop(0, sources, place, 0)
    for ref, at in ((top_ref, EDGE - 8), (low_ref, EDGE + height)):
        for b in range(blocks):
            for k in range(TIERS):
                t[0, k, b, at : at + 8] = ref[k * blocks + b]
            dens[b, at : at + 8] = ref[TIERS * blocks + b]
        for i in range(2):
            s[0, i, at : at + 8] = ref[(TIERS + 1) * blocks]
            side[i, at : at + 8] = ref[(TIERS + 1) * blocks + 1]

    share_lane = by_lane(share)

    def strips(n, carry):
        at = pl.multiple_of(EDGE - 8 + 8 * n, 8)
        for i, b in ((0, 0), (1, blocks - 1)):
            halo = (inner < 8) if i == 0 else (inner >= 8)
            warm = jnp.zeros((8, LANES), jnp.float32)
            power = jnp.zeros((8, LANES), jnp.float32)
            full = dens[b, pl.ds(at, 8)]
            for k in range(TIERS):
                turn = (16 * k + 8) % LANES
                warm = jnp.where(group == k, pltpu.roll(t[0, k, b, pl.ds(at, 8)], turn, 1), warm)
                power = jnp.where(group == k, pltpu.roll(full, turn, 1), power)
            s[0, i, pl.ds(at, 8)] = jnp.where(halo, s[0, i, pl.ds(at, 8)], warm)
            side[i, pl.ds(at, 8)] = share_lane * jnp.where(halo, side[i, pl.ds(at, 8)], power)
        return carry

    lax.fori_loop(0, height // 8 + 2, strips, 0)

    lat_lane = by_lane(lat)
    own_lane = by_lane(own)
    up_lane = by_lane(ver[:-1] + [0.0])
    down_lane = by_lane([0.0] + ver[:-1])
    dead = (inner < 8 * edge_ref[2], inner >= 16 - 8 * edge_ref[3])

    def advance(now, new, at):
        rows = pl.ds(at, 8)
        above, below = pl.ds(at - 1, 8), pl.ds(at + 1, 8)
        sides = []
        for i in range(2):
            c = s[now, i, rows]
            around = (s[now, i, above] + s[now, i, below]) + (pltpu.roll(c, 1, 1) + pltpu.roll(c, LANES - 1, 1))
            fresh = own_lane * c + lat_lane * around + side[i, rows]
            fresh = fresh + up_lane * pltpu.roll(c, LANES - 16, 1) + down_lane * pltpu.roll(c, 16, 1)
            s[new, i, rows] = jnp.where(dead[i], 0.0, fresh)
            sides.append(c)
        power = [dens[b, rows] for b in range(blocks)]
        here = [t[now, 0, b, rows] for b in range(blocks)]
        under = None
        for k in range(TIERS):
            over = [t[now, k + 1, b, rows] for b in range(blocks)] if k + 1 < TIERS else None
            right = [pltpu.roll(c, 1, 1) for c in here]
            left = [pltpu.roll(c, LANES - 1, 1) for c in here]
            first = pltpu.roll(sides[0], (121 - 16 * k) % LANES, 1)
            last = pltpu.roll(sides[1], (119 - 16 * k) % LANES, 1)
            for b in range(blocks):
                c = here[b]
                west = jnp.where(lane == 0, right[b - 1] if b else first, right[b])
                east = jnp.where(lane == LANES - 1, left[b + 1] if b + 1 < blocks else last, left[b])
                around = (t[now, k, b, above] + t[now, k, b, below]) + (west + east)
                fresh = (own[k] * c + lat[k] * around) + share[k] * power[b]
                if over is not None:
                    fresh = fresh + ver[k] * over[b]
                if under is not None:
                    fresh = fresh + ver[k - 1] * under[b]
                t[new, k, b, rows] = fresh
            under, here = here, over

    def clear(new, at):
        zero = jnp.zeros((8, LANES), jnp.float32)
        for b in range(blocks):
            for k in range(TIERS):
                t[new, k, b, at : at + 8] = zero
        for i in range(2):
            s[new, i, at : at + 8] = zero

    def step(n, carry):
        now = n % 2
        new = 1 - now

        def row(i, inner_carry):
            advance(now, new, pl.multiple_of(EDGE - 8 + 8 * i, 8))
            return inner_carry

        lax.fori_loop(0, height // 8 + 2, row, 0)

        @pl.when(at_top)
        def _():
            clear(new, EDGE - 8)

        @pl.when(at_low)
        def _():
            clear(new, EDGE + height)

        return carry

    lax.fori_loop(0, STEPS - 1, step, 0)

    now = (STEPS - 1) % 2
    new = 1 - now
    pieces = 4
    tall = height // pieces
    copies = []
    for n in range(pieces):

        def row(i, carry, n=n):
            advance(now, new, pl.multiple_of(EDGE + n * tall + 8 * i, 8))
            return carry

        lax.fori_loop(0, tall // 8, row, 0)
        for b in range(blocks):
            copy = pltpu.make_async_copy(
                t.at[new, :, b, pl.ds(EDGE + n * tall, tall)],
                out_ref.at[:, pl.ds(n * tall, tall), pl.ds(b * LANES, LANES)],
                sems.at[n, b],
            )
            copy.start()
            copies.append(copy)
    for copy in copies:
        copy.wait()


def run_steps(edges, materials, lateral, vertical, heating, got, top, low):
    sources, parts, strip, _ = got.shape
    blocks = (parts - 2) // (TIERS + 1)
    height = sources * strip
    tall = height + 2 * EDGE
    return pl.pallas_call(
        step_kernel,
        out_shape=jax.ShapeDtypeStruct((TIERS, height, blocks * LANES), jnp.float32),
        in_specs=[pl.BlockSpec(memory_space=SMEM)] * 5 + [pl.BlockSpec(memory_space=VMEM)] * 3,
        out_specs=pl.BlockSpec(memory_space=pl.ANY),
        scratch_shapes=[
            pltpu.VMEM((2, TIERS, blocks, tall, LANES), jnp.float32),
            pltpu.VMEM((2, 2, tall, LANES), jnp.float32),
            pltpu.VMEM((blocks, tall, LANES), jnp.float32),
            pltpu.VMEM((2, tall, LANES), jnp.float32),
            pltpu.SemaphoreType.DMA((4, blocks)),
        ],
        compiler_params=pltpu.CompilerParams(vmem_limit_bytes=40 << 20),
    )(edges, materials, lateral, vertical, heating, got, top, low)


def body(heat, labels, flux, materials, lateral, vertical, heating):
    row_count = lax.axis_size("rows")
    col_count = lax.axis_size("cols")
    r, c = lax.axis_index("rows"), lax.axis_index("cols")
    blocks = heat.shape[2] // col_count // LANES
    sent = pack(heat, labels, flux[None, :], col_count, blocks)
    got = lax.all_to_all(sent, "cols", split_axis=0, concat_axis=0, tiled=True)
    down = [(i, i + 1) for i in range(row_count - 1)]
    top = lax.ppermute(got[-1, :, -8:], "rows", down)
    low = lax.ppermute(got[0, :, :8], "rows", [(b, a) for a, b in down])
    edges = jnp.stack([r == 0, r == row_count - 1, c == 0, c == col_count - 1]).astype(jnp.int32)
    return run_steps(edges, materials, lateral, vertical, heating, got, top, low)


def solution(mesh):
    return jax.shard_map(
        body,
        mesh=mesh,
        in_specs=(P(None, ("rows", "cols"), None), P(("rows", "cols"), None), P(), P(), P(), P(), P()),
        out_specs=P(None, "rows", "cols"),
        check_vma=False,
    )
```
